32 devices in a mesh: groups: 2 (over y), rows: 4 (over z), cols: 2 (over x), sub: 2 (over core).
Axes of the slice: x: 2, y: 2, z: 4, core: 2. Of those that a mesh axis runs over, the one named last changes fastest.
Arguments:
- stored_vectors: bfloat16 [3072, 8192], P(('cols', 'sub'), ('groups', 'rows')), parts along dimension 1, may hold values from -0.59765625 to 0.59765625
- previous_columns: bfloat16 [8192, 256], P(('groups', 'rows', 'cols', 'sub')), parts along dimension 0, may hold values from -3 to 3
- pivots: int32 [512], P('groups'), parts along dimension 0, may hold values from 0 to 4095, as said below
- diagonal: float32 [8192], P(('groups', 'rows', 'cols', 'sub')), parts along dimension 0, may hold values from 2 to 32
- ket_blocks: bfloat16 [128, 128, 256], P(('groups', 'rows', 'cols', 'sub')), parts along dimension 0, may hold values from -6 to 6
- shell_tags: int32 [128, 128], P(('groups', 'rows', 'cols', 'sub')), parts along dimension 0, may hold values from 0 to 3
- target_blocks: int32 [32, 4], P('groups'), parts along dimension 0, may hold values from 0 to 31, as said below
- block_counts: int32 [32], P('groups'), parts along dimension 0, may hold values from 0 to 4, as said below
- shell_norms: float32 [4], replicated, may hold values from 0.5 to 2
Outputs:
- new_vectors: bfloat16 [8192, 256], P(('groups', 'rows', 'cols', 'sub')), parts along dimension 0
- diag_out: float32 [8192], P(('groups', 'rows', 'cols', 'sub')), parts along dimension 0
- next_columns: bfloat16 [8192, 256], P(('groups', 'rows', 'cols', 'sub')), parts along dimension 0
The draws below stay inside these ranges and needn't reach their ends.
There are 2 independent parts, one for each index of `groups`. The reference program is written for one: setup_inputs(seed, part) draws one part's arguments, and reference() takes and returns one part's arrays. A program takes and returns all parts, laid end to end along the dimension named above; an argument that names none is the same for every part. Nothing has to cross between parts.
Inputs may be any that keep to these rules, and one draw needn't show every extreme that they name: `pivots`: 256 distinct AO pairs. `target_blocks`: the used slots of all owners name every block of the 32 blocks exactly once; a used slot's block lies on a device with the owner's cols and sub indices (blocks g * 2 to g * 2 + 1 lie on the device of linear index g, rows slowest; owner o is the device of linear index o). At most 1 of one owner's used slots go to one device, and some owner reaches that in every draw. Entries of unused slots are arbitrary blocks. `block_counts`: some owner uses all 4 slots in every draw.
All inputs are finite; a program needn't handle non-finite values.
Results may differ from the reference program's by a relative error of at most 0.0004.
Values may be sent and summed in bfloat16 or wider, within the bound.
No kernel may reach another device: no remote copies, remote signals or barrier semaphores. Data moves between devices by JAX's collectives and lax.ppermute only.
A program may use at most 64 MiB of HBM per device.

```python
import math
import jax
import jax.numpy as jnp
from jax import lax

K = 3072
B = 256
BLK = 128
BLOCKS_DEV = 2
SHELL_TYPES = 4
CAP = 4
OWNERS = 16
PAIRS = 4096
N_ROWS = 4
N_COLS = 2
N_SUB = 2


def layout_draw(key):
    band_count = N_ROWS
    column = N_COLS * N_SUB
    per_device = BLOCKS_DEV
    slot_count = 2 * BLOCKS_DEV
    base = jax.random.fold_in(key, 11)
    keys = jax.random.split(base, 4)
    ranks = jnp.arange(band_count, dtype=jnp.int32)
    rank_counts = jnp.where(ranks == 0, slot_count, jnp.where(ranks == 1, 0, per_device)).astype(jnp.int32)
    rank_starts = (jnp.cumsum(rank_counts) - rank_counts).astype(jnp.int32)
    order = jax.vmap(lambda sub_key: jax.random.permutation(sub_key, band_count))(jax.random.split(keys[0], column)).astype(jnp.int32)
    lines = jnp.arange(column, dtype=jnp.int32)[:, None]
    counts = jnp.zeros((column, band_count), jnp.int32).at[lines, order].set(jnp.broadcast_to(rank_counts, (column, band_count)))
    starts = jnp.zeros((column, band_count), jnp.int32).at[lines, order].set(jnp.broadcast_to(rank_starts, (column, band_count)))
    total = band_count * per_device
    receiver_order = jax.vmap(lambda sub_key: jax.random.permutation(sub_key, band_count))(jax.random.split(keys[1], column)).astype(jnp.int32)
    within_order = jax.vmap(lambda sub_key: jax.random.permutation(sub_key, per_device))(jax.random.split(keys[2], column)).astype(jnp.int32)
    slots = jnp.arange(slot_count, dtype=jnp.int32)
    position = jnp.minimum(starts[:, :, None] + slots[None, None, :], total - 1)
    receiver_spread = jnp.broadcast_to(receiver_order[:, None, :], (column, band_count, band_count))
    receiver = jnp.take_along_axis(receiver_spread, position % band_count, axis=2)
    within_spread = jnp.broadcast_to(within_order[:, None, :], (column, band_count, per_device))
    within = jnp.take_along_axis(within_spread, position // band_count, axis=2)
    target = (receiver * column + jnp.arange(column, dtype=jnp.int32)[:, None, None]) * per_device + within
    filler = jax.random.randint(keys[3], (column, band_count, slot_count), 0, band_count * column * per_device).astype(jnp.int32)
    valid = slots[None, None, :] < counts[:, :, None]
    target = jnp.where(valid, target, filler)
    target = jnp.transpose(target, (1, 0, 2)).reshape(band_count * column, slot_count)
    owner_counts = jnp.transpose(counts, (1, 0)).reshape(band_count * column)
    return (target.astype(jnp.int32), owner_counts.astype(jnp.int32))


def draw_target_blocks(key, part):
    return layout_draw(key)[0]


def draw_block_counts(key, part):
    return layout_draw(key)[1]


def draw_pivots(key, part):
    chosen = jax.random.permutation(jax.random.fold_in(key, 5), PAIRS)
    return chosen[:B].astype(jnp.int32)


def place_ends(entries, key, smallest, largest):
    longest = entries.shape.index(max(entries.shape))
    spots = []
    for shift in (0, 1):
        where = [jax.random.randint(jax.random.fold_in(key, axis), (), 0, length) for axis, length in enumerate(entries.shape)]
        where[longest] = (where[longest] + shift) % entries.shape[longest]
        spots.append(tuple(where))
    return entries.at[spots[0]].set(smallest).at[spots[1]].set(largest)


def block_levels(rng, extent, cuts, low, high):
    gain = 1.0
    for dim, shards_of in cuts:
        draws = jax.random.uniform(jax.random.fold_in(jax.random.fold_in(rng, 6), dim), (shards_of,), jnp.float32, low / len(cuts), high / len(cuts))
        gain = gain * jnp.repeat(jnp.exp(draws), extent[dim] // shards_of).reshape((-1,) + (1,) * (len(extent) - 1 - dim))
    return gain


def centred(own_key, extent, scale, most, pieces=(), kind=jnp.bfloat16):
    entries = scale * jax.random.normal(own_key, extent, jnp.float32)
    if pieces:
        entries = entries * block_levels(own_key, extent, pieces, -0.22, 0.18)
    return jnp.clip(entries, -most, most).astype(kind)


def setup_inputs(seed: int = 0, part: int = 0) -> dict:
    seeds = jax.random.split(jax.random.key(seed), 10)
    part_keys = jax.random.split(jax.random.fold_in(seeds[9], part), 10)
    return {
        "stored_vectors": centred(part_keys[0], (K, PAIRS), 0.1, 0.59765625, ((0, 4), (1, 4))),
        "previous_columns": centred(part_keys[1], (PAIRS, B), 0.5, 3.0, ((0, 16),)),
        "pivots": draw_pivots(jax.random.fold_in(jax.random.fold_in(seeds[9], part), 71), part),
        "diagonal": jnp.clip(jnp.exp(math.log(32.0) - 2.7725887 * jax.random.uniform(part_keys[3], (PAIRS,), jnp.float32) ** block_levels(part_keys[3], (PAIRS,), ((0, 16),), -0.2, 0.2)), 2.0, 32.0),
        "ket_blocks": centred(part_keys[4], (OWNERS * CAP, BLK, B), 1.0, 6.0, ((0, 16),)),
        "shell_tags": place_ends(jax.random.randint(part_keys[5], (OWNERS * CAP, BLK), 0, SHELL_TYPES), jax.random.fold_in(part_keys[5], 1), 0, SHELL_TYPES - 1).astype(jnp.int32),
        "target_blocks": draw_target_blocks(jax.random.fold_in(jax.random.fold_in(seeds[9], part), 71), part),
        "block_counts": draw_block_counts(jax.random.fold_in(jax.random.fold_in(seeds[9], part), 71), part),
        "shell_norms": jnp.clip(jnp.exp(jax.random.uniform(seeds[8], (SHELL_TYPES,), jnp.float32, math.log(0.5), math.log(2.0))), 0.5, 2.0),
    }


def reference(stored_vectors, previous_columns, pivots, diagonal, ket_blocks, shell_tags, target_blocks, block_counts, shell_norms):
    kinds = jnp.arange(shell_norms.shape[0], dtype=jnp.int32)
    factor = lax.optimization_barrier(jnp.sum(jnp.where(shell_tags[..., None] == kinds, shell_norms, jnp.float32(0.0)), axis=-1))
    fresh = (ket_blocks.astype(jnp.float32) * factor[..., None]).astype(jnp.bfloat16)
    slots = jnp.arange(CAP, dtype=jnp.int32)
    valid = slots[None, :] < block_counts[:, None]
    blocks_total = PAIRS // BLK
    placing = jnp.where(valid, target_blocks, blocks_total).reshape(-1).astype(jnp.int32)
    placed = jnp.zeros((blocks_total, BLK, B), jnp.bfloat16).at[placing].set(fresh, mode='drop')
    next_columns = placed.reshape(PAIRS, B)
    pivot_rows = stored_vectors[:, pivots]
    groups_count = N_COLS * N_SUB
    width = K // groups_count
    product = jnp.zeros((PAIRS, B), jnp.float32)
    for group in range(groups_count):
        block_vectors = stored_vectors[group * width:(group + 1) * width]
        block_pivots = pivot_rows[group * width:(group + 1) * width]
        partial_sum = jnp.dot(block_vectors.T, block_pivots, preferred_element_type=jnp.float32)
        product = product + partial_sum
    residual_cols = previous_columns.astype(jnp.float32) - product
    pivot_diag = diagonal[pivots]
    scaled = residual_cols / jnp.sqrt(pivot_diag)[None, :]
    new_vectors = scaled.astype(jnp.bfloat16)
    diag_out = diagonal - lax.optimization_barrier(jnp.sum(scaled * scaled, axis=1))
    return (new_vectors, diag_out, next_columns)
```

```python
import functools
import math
import jax
import jax.numpy as jnp
from jax import lax
from jax.experimental import pallas as pl
from jax.experimental.pallas import tpu as pltpu
from jax.sharding import PartitionSpec as P

F32 = jnp.float32
BF16 = jnp.bfloat16
I32 = jnp.int32
LANES = 128
SPARE = 3
VMEM = pl.BlockSpec(memory_space=pltpu.VMEM)
SMEM = pl.BlockSpec(memory_space=pltpu.SMEM)


def slots_of(batch, bands):
    mean = batch / bands
    return min(
        -(-(batch + SPARE) // 16) * 16,
        -(-int(mean + 3.6 * math.sqrt(mean) + SPARE) // 16) * 16,
    )


def nt(a, b):
    return lax.dot_general(a, b, (((1,), (1,)), ((), ())), preferred_element_type=F32)


def tn(a, b):
    return lax.dot_general(a, b, (((0,), (0,)), ((), ())), preferred_element_type=F32)


def split3(x):
    high = x.astype(BF16)
    rest = x - high.astype(F32)
    mid = rest.astype(BF16)
    low = (rest - mid.astype(F32)).astype(BF16)
    return high, mid, low


def ranks_in(mask):
    batch = mask.shape[1]
    above = lax.broadcasted_iota(I32, (batch, batch), 0) < lax.broadcasted_iota(
        I32, (batch, batch), 1
    )
    return jnp.dot(mask.astype(BF16), above.astype(BF16), preferred_element_type=F32)


def select_kernel(place_ref, pivots_ref, diag_ref, vectors_ref, out_ref, *, slots):
    cap = slots - SPARE
    width, band_rows = vectors_ref.shape
    batch = pivots_ref.shape[1]
    rows_here = diag_ref.shape[1]
    padded = -(-slots // LANES) * LANES
    band = place_ref[0]
    column = place_ref[1]
    local = pivots_ref[...] - band * band_rows
    mine = (local >= 0) & (local < band_rows)
    rank = ranks_in(jnp.broadcast_to(jnp.where(mine, 1.0, 0.0), (8, batch)))[0:1]
    rank = rank.astype(I32) - place_ref[4]
    line = lax.broadcasted_iota(I32, (padded, batch), 0)
    hit = (rank == line) & mine & (line < cap)
    where = jnp.sum(jnp.where(hit, (local + 1).astype(F32), 0.0), axis=1, keepdims=True)
    where = where.astype(I32) - 1
    chosen = where[:slots] == lax.broadcasted_iota(I32, (slots, band_rows), 1)
    picked = nt(jnp.where(chosen, 1.0, 0.0).astype(BF16), vectors_ref[...])
    out_ref[...] = picked.astype(BF16)
    own = where == column * rows_here + lax.broadcasted_iota(I32, (padded, rows_here), 1)
    high, mid, low = split3(diag_ref[...])
    row = lax.broadcasted_iota(I32, (16, rows_here), 0)
    diag = jnp.where(
        row == 13,
        high.astype(F32),
        jnp.where(row == 14, mid.astype(F32), jnp.where(row == 15, low.astype(F32), 0.0)),
    ).astype(BF16)
    spare = nt(diag, jnp.where(own, 1.0, 0.0).astype(BF16))
    out_ref[slots - 16 :, 0:padded] = (picked[slots - 16 :, 0:padded] + spare).astype(BF16)


def multiply_kernel(place_ref, *refs, pieces, slots, cols, sub, rows_here):
    piece_refs, vectors_ref, keep_ref, send_ref = (
        refs[:pieces],
        refs[pieces],
        refs[pieces + 1],
        refs[pieces + 2],
    )
    padded = -(-slots // LANES) * LANES
    mine_c = place_ref[2]
    mine_s = place_ref[3]
    left = jnp.concatenate([ref[...] for ref in piece_refs], axis=0)
    row = lax.broadcasted_iota(I32, (8, padded), 0)
    for out_ref, way in ((keep_ref, 0), (send_ref, 1)):
        for step in range(cols):
            block = (mine_c ^ step) * sub + (mine_s ^ way)
            start = pl.multiple_of(block * rows_here, LANES)
            got = jnp.dot(
                left, vectors_ref[:, pl.ds(start, rows_here)], preferred_element_type=F32
            )
            at = step * rows_here
            out_ref[:, at : at + rows_here] = got
            for piece in range(pieces):
                low = (piece + 1) * slots - 8
                spare = left[low - 8 : low + 8, 0:padded].astype(F32)[8:16]
                out_ref[low : low + 8, at : at + padded] = jnp.where(
                    row >= 8 - SPARE, spare, got[low : low + 8, 0:padded]
                )


def gather_terms(place_ref, pivots_ref, refs, groups, slots, bands, band_rows, rows_here, offset):
    batch = pivots_ref.shape[1]
    cap = slots - SPARE
    padded = -(-slots // LANES) * LANES
    band = place_ref[0]
    pivots = pivots_ref[...]
    lines = -(-bands // 8) * 8
    number = lax.broadcasted_iota(I32, (lines, batch), 0)
    inside = (pivots >= number * band_rows) & (pivots < (number + 1) * band_rows)
    inside = jnp.where(inside, 1.0, 0.0)
    ranks = ranks_in(inside)
    rank = jnp.sum(inside * ranks, axis=0, keepdims=True).astype(I32) - offset
    home = jnp.sum(inside * number.astype(F32), axis=0, keepdims=True).astype(I32)
    line = lax.broadcasted_iota(I32, (padded, batch), 0)
    product = jnp.zeros((rows_here, batch), F32)
    spare = jnp.zeros((8, batch), F32)
    used = 0
    for sources, count in groups:
        total = refs[used][:, 0:rows_here]
        for ref in refs[used + 1 : used + count]:
            total = total + ref[:, 0:rows_here]
        used += count
        for piece, step in enumerate(sources):
            part = total[piece * slots : (piece + 1) * slots]
            spot = jnp.where(home == (band ^ step), rank, -1)
            place = jnp.where((line == spot) & (line < cap), 1.0, 0.0).astype(BF16)
            for term in split3(part):
                product = product + tn(term, place[:slots])
            spare = spare + jnp.dot(
                part[slots - 8 :, 0:padded].astype(BF16), place, preferred_element_type=F32
            )
    return product, spare


def add_kernel(place_ref, pivots_ref, product_ref, spare_ref, *refs, **sizes):
    product, spare = gather_terms(
        place_ref,
        pivots_ref,
        refs[:-2],
        rows_here=product_ref.shape[0],
        offset=place_ref[4],
        **sizes,
    )
    refs[-2][...] = product_ref[...] + product
    refs[-1][...] = spare_ref[...] + spare


def finish_kernel(place_ref, pivots_ref, diag_ref, previous_ref, *refs, extra, **sizes):
    new_ref, diag_out_ref = refs[-2:]
    rows_here = diag_ref.shape[1]
    product, spare = gather_terms(
        place_ref, pivots_ref, refs[extra:-2], rows_here=rows_here, offset=0, **sizes
    )
    if extra:
        product = product + refs[0][...]
        spare = spare + refs[1][...]
    pivot_diag = jnp.sum(spare[8 - SPARE :], axis=0, keepdims=True)
    scaled = (previous_ref[...].astype(F32) - product) * (1.0 / jnp.sqrt(pivot_diag))
    new_ref[...] = scaled.astype(BF16)
    sums = jnp.sum(scaled * scaled, axis=1, keepdims=True)
    same = lax.broadcasted_iota(I32, (rows_here, rows_here), 0) == lax.broadcasted_iota(
        I32, (rows_here, rows_here), 1
    )
    turned = jnp.sum(jnp.where(same, sums, 0.0), axis=0, keepdims=True)
    diag_out_ref[...] = diag_ref[...] - turned


def ket_kernel(place_ref, norms_ref, targets_ref, counts_ref, tags_ref, ket_ref, out_ref, *, per_device, column_size):
    me = place_ref[0] * column_size + place_ref[1]
    tags = tags_ref[...]
    slot_count = tags.shape[0]
    factor = jnp.zeros(tags.shape, F32)
    for kind in range(norms_ref.shape[0]):
        factor = jnp.where(tags == kind, norms_ref[kind], factor)
    fill = -(-slot_count // 8) * 8 - slot_count
    if fill:
        factor = jnp.concatenate([factor, jnp.zeros((fill, tags.shape[1]), F32)], axis=0)
    factor = factor.T
    for slot in range(slot_count):
        fresh = (ket_ref[slot].astype(F32) * factor[:, slot : slot + 1]).astype(BF16)
        receiver = targets_ref[me, slot] // (column_size * per_device)

        @pl.when(slot < counts_ref[me])
        def _():
            out_ref[receiver] = fresh


def place_kernel(place_ref, targets_ref, counts_ref, incoming_ref, out_ref, *, per_device, column_size):
    me = place_ref[0] * column_size + place_ref[1]
    block_rows = incoming_ref.shape[1]
    for source in range(incoming_ref.shape[0]):
        owner = source * column_size + place_ref[1]
        for slot in range(targets_ref.shape[1]):
            block = targets_ref[owner, slot]

            @pl.when((slot < counts_ref[owner]) & (block // per_device == me))
            def _():
                start = pl.multiple_of((block % per_device) * block_rows, block_rows)
                out_ref[pl.ds(start, block_rows), :] = incoming_ref[source]


def call(kernel, outs, specs, args, name):
    return pl.pallas_call(
        kernel,
        out_shape=outs,
        in_specs=specs,
        out_specs=jax.tree.map(lambda _: VMEM, outs),
        name=name,
    )(*args)


def body(
    stored_vectors,
    previous_columns,
    pivots,
    diagonal,
    ket_blocks,
    shell_tags,
    target_blocks,
    block_counts,
    shell_norms,
    *,
    bands,
    cols,
    sub,
):
    rows_here, batch = previous_columns.shape
    width, band_rows = stored_vectors.shape
    block_rows = ket_blocks.shape[1]
    per_device = rows_here // block_rows
    slots = slots_of(batch, bands)
    cap = slots - SPARE
    band_index = lax.axis_index("rows")
    cols_index = lax.axis_index("cols")
    sub_index = lax.axis_index("sub")
    place = jnp.stack(
        [band_index, cols_index * sub + sub_index, cols_index, sub_index, jnp.int32(0)]
    ).astype(I32)
    pivot_line = pivots.reshape(1, batch)
    diag_line = diagonal.reshape(1, rows_here)

    def swap(x, axis, size, step):
        return lax.ppermute(x, axis, [(i, i ^ step) for i in range(size)])

    def select(where):
        return call(
            functools.partial(select_kernel, slots=slots),
            jax.ShapeDtypeStruct((slots, width), BF16),
            [SMEM, VMEM, VMEM, VMEM],
            (where, pivot_line, diag_line, stored_vectors),
            "select",
        )

    def reduce_group(pieces):
        count = len(pieces)
        out = jax.ShapeDtypeStruct((count * slots, cols * rows_here), F32)
        keep, send = call(
            functools.partial(
                multiply_kernel,
                pieces=count,
                slots=slots,
                cols=cols,
                sub=sub,
                rows_here=rows_here,
            ),
            (out, out),
            [SMEM] + [VMEM] * (count + 1),
            (place, *pieces, stored_vectors),
            "multiply",
        )
        terms = [keep, swap(send, "sub", sub, 1)]
        step = cols // 2
        while step:
            at = step * rows_here
            upper = terms[0][:, at : 2 * at]
            for term in terms[1:]:
                upper = upper + term[:, at : 2 * at]
            terms.append(swap(upper, "cols", cols, step))
            step //= 2
        return terms

    def settings(groups):
        meta = tuple((sources, len(terms)) for sources, terms in groups)
        arrays = [term for _, terms in groups for term in terms]
        return dict(groups=meta, slots=slots, bands=bands, band_rows=band_rows), arrays

    def finish(groups, before=()):
        sizes, arrays = settings(groups)
        arrays = [*before, *arrays]
        return call(
            functools.partial(finish_kernel, extra=len(before), **sizes),
            (
                jax.ShapeDtypeStruct((rows_here, batch), BF16),
                jax.ShapeDtypeStruct((1, rows_here), F32),
            ),
            [SMEM] + [VMEM] * (3 + len(arrays)),
            (place, pivot_line, diag_line, previous_columns, *arrays),
            "finish",
        )

    def gather(own):
        order = sorted(range(1, bands), key=lambda d: (d != bands - 1, d))
        return {0: own, **{d: swap(own, "rows", bands, d) for d in order}}

    held = gather(select(place))
    rest = tuple(range(2, bands))
    main = [(0,), (1,)][:bands] + ([rest] if rest else [])
    groups = [(s, reduce_group([held[d] for d in s])) for s in main]

    outgoing = call(
        functools.partial(ket_kernel, per_device=per_device, column_size=cols * sub),
        jax.ShapeDtypeStruct((bands,) + ket_blocks.shape[1:], BF16),
        [SMEM, SMEM, SMEM, SMEM, VMEM, VMEM],
        (place, shell_norms, target_blocks, block_counts, shell_tags, ket_blocks),
        "ket",
    )
    if bands > 1:
        outgoing, _ = lax.optimization_barrier((outgoing, held[bands - 1]))
    incoming = lax.all_to_all(outgoing, "rows", split_axis=0, concat_axis=0, tiled=True)
    next_columns = call(
        functools.partial(place_kernel, per_device=per_device, column_size=cols * sub),
        jax.ShapeDtypeStruct((rows_here, batch), BF16),
        [SMEM, SMEM, SMEM, VMEM],
        (place, target_blocks, block_counts, incoming),
        "place",
    )

    def plain():
        return finish(groups)

    def further():
        every = tuple(range(bands))

        def step(number, sums):
            where = place.at[4].set(number * cap)
            pieces = gather(select(where))
            sizes, arrays = settings([(every, reduce_group([pieces[d] for d in every]))])
            return call(
                functools.partial(add_kernel, **sizes),
                tuple(jax.ShapeDtypeStruct(x.shape, F32) for x in sums),
                [SMEM] + [VMEM] * (3 + len(arrays)),
                (where, pivot_line, *sums, *arrays),
                "add",
            )

        start = (jnp.zeros((rows_here, batch), F32), jnp.zeros((8, batch), F32))
        return finish(groups, lax.fori_loop(1, -(-batch // cap), step, start))

    if cap < batch:
        homes = pivots // band_rows
        held_by = jnp.sum(
            (homes[None, :] == jnp.arange(bands, dtype=I32)[:, None]).astype(I32), axis=1
        )
        new_vectors, diag_out = lax.cond(jnp.max(held_by) > cap, further, plain)
    else:
        new_vectors, diag_out = plain()
    return (new_vectors, diag_out.reshape(rows_here), next_columns)


def solution(mesh):
    sizes = dict(mesh.shape)
    return jax.shard_map(
        functools.partial(body, bands=sizes["rows"], cols=sizes["cols"], sub=sizes["sub"]),
        mesh=mesh,
        in_specs=(
            P(("cols", "sub"), ("groups", "rows")),
            P(("groups", "rows", "cols", "sub"), None),
            P("groups"),
            P(("groups", "rows", "cols", "sub")),
            P(("groups", "rows", "cols", "sub"), None, None),
            P(("groups", "rows", "cols", "sub"), None),
            P("groups", None),
            P("groups"),
            P(),
        ),
        out_specs=(
            P(("groups", "rows", "cols", "sub"), None),
            P(("groups", "rows", "cols", "sub")),
            P(("groups", "rows", "cols", "sub"), None),
        ),
        check_vma=False,
    )
```
